32 devices in a mesh: chip: 2 (over y), board: 4 (over z), cuts: 4 (over x, core).
Axes of the slice: x: 2, y: 2, z: 4, core: 2. Of those that a mesh axis runs over, the one named last changes fastest.
Arguments:
- features: bfloat16 [32, 2048, 1024], P(('chip', 'board', 'cuts')), may hold values from -6 to 6
- targets: bfloat16 [32, 2048, 256], P(('chip', 'board', 'cuts')), may hold values from -24 to 24
- lower_weight: bfloat16 [32, 1024, 512], P(('chip', 'board', 'cuts')), may hold values from -0.1875 to 0.1875
- head_weight: float32 [32, 512, 256], P(('chip', 'board', 'cuts')), may hold values from -0.25 to 0.25
- batch_rows: int32 [32, 2, 1024], P(('chip', 'board', 'cuts')), may hold values from 0 to 2047
- sample_counts: int32 [32], P(('chip', 'board', 'cuts')), may hold values from 1 to 1000
- cluster_ids: int32 [32], P(('chip', 'board', 'cuts')), may hold values from 0 to 7, as said below
Outputs:
- cluster_step: float32 [32, 512, 256], P(('chip', 'board', 'cuts'))
The draws below stay inside these ranges and needn't reach their ends.
Inputs may be any that keep to these rules, and one draw needn't show every extreme that they name: `cluster_ids`: every one of the 8 clusters has at least one client.
All inputs are finite; a program needn't handle non-finite values.
Results may differ from the reference program's by a relative error of at most 0.0003.
Values sent between devices are 32-bit elements; how exact they have to be, the bound alone decides.
A program may use at most 64 MiB of HBM per device.

```python
import jax
import jax.numpy as jnp
from jax import lax

IN = 1024
HID = 512
OUT = 256
CLUSTERS = 8
STEPS = 2
POOL = 2048
ROWS = 1024
CLIENTS = 32


def draw_cluster_ids(key, part):
    first = jax.random.fold_in(key, 11)
    second = jax.random.fold_in(key, 23)
    drawn = jax.random.randint(first, (CLIENTS,), 0, CLUSTERS, dtype=jnp.int32)
    order = jax.random.permutation(second, CLIENTS)
    return drawn.at[order[:CLUSTERS]].set(jnp.arange(CLUSTERS, dtype=jnp.int32))


def with_ends(values, rng, smallest, largest):
    index_at = [jax.random.randint(jax.random.fold_in(rng, axis), (), 0, length) for axis, length in enumerate(values.shape)]
    widest = values.shape.index(max(values.shape))
    neighbour = index_at[:widest] + [(index_at[widest] + 1) % values.shape[widest]] + index_at[widest + 1:]
    return values.at[tuple(index_at)].set(smallest).at[tuple(neighbour)].set(largest)


def level_of(key, shape, cuts, low, largest):
    def one(dim, parts):
        draws = jax.random.uniform(jax.random.fold_in(jax.random.fold_in(key, 6), dim), (parts,), jnp.float32, low / len(cuts), largest / len(cuts))
        return jnp.repeat(jnp.exp(draws), shape[dim] // parts).reshape((-1,) + (1,) * (len(shape) - dim - 1))

    gain = one(*cuts[0])
    for cut in cuts[1:]:
        gain = gain * one(*cut)
    return gain


def centred(key, shape, width, limit, cuts=(), kind=jnp.bfloat16):
    result = jax.random.normal(key, shape, jnp.float32) * width
    if len(cuts) > 0:
        result = level_of(key, shape, cuts, -0.22, 0.18) * result
    return jnp.clip(result, min=-limit, max=limit).astype(kind)


def setup_inputs(seed: int = 0) -> dict:
    arg_keys = jax.random.split(jax.random.key(seed), 8)
    return {
        "features": centred(arg_keys[0], (CLIENTS, POOL, IN), 1.0, 6.0, ((0, 32),)),
        "targets": centred(arg_keys[1], (CLIENTS, POOL, OUT), 4.0, 24.0, ((0, 32),)),
        "lower_weight": centred(arg_keys[2], (CLIENTS, IN, HID), IN ** -0.5, 0.1875, ((0, 32),)),
        "head_weight": centred(arg_keys[3], (CLIENTS, HID, OUT), HID ** -0.5, 0.25, ((0, 32),), jnp.float32),
        "batch_rows": with_ends(jax.random.randint(arg_keys[4], (CLIENTS, STEPS, ROWS), 0, POOL), jax.random.fold_in(arg_keys[4], 1), 0, POOL - 1).astype(jnp.int32),
        "sample_counts": with_ends(jax.random.randint(arg_keys[5], (CLIENTS,), 1, 1001), jax.random.fold_in(arg_keys[5], 1), 1, 1000).astype(jnp.int32),
        "cluster_ids": draw_cluster_ids(jax.random.fold_in(arg_keys[7], 71), 0),
    }


LR = 0.5


def one_client(args):
    feats, targs, lower, head, rows = args
    hidden = jnp.tanh(jnp.dot(feats, lower, preferred_element_type=jnp.float32))
    weight = head
    for step in range(STEPS):
        picked = jnp.take(hidden, rows[step], axis=0)
        wanted = jnp.take(targs, rows[step], axis=0).astype(jnp.float32)
        err = jnp.dot(picked, weight, precision=lax.Precision.HIGHEST) - wanted
        grad = jnp.dot(picked.T, err, precision=lax.Precision.HIGHEST) / ROWS
        weight = weight - LR * grad
    return weight - head


def reference(features, targets, lower_weight, head_weight, batch_rows, sample_counts, cluster_ids):
    deltas = lax.map(one_client, (features, targets, lower_weight, head_weight, batch_rows))
    onehot = (cluster_ids[:, None] == jnp.arange(CLUSTERS, dtype=jnp.int32)[None, :]).astype(jnp.float32)
    weighted = onehot * sample_counts.astype(jnp.float32)[:, None]
    flat = deltas.reshape(CLIENTS, HID * OUT)
    sums = jnp.dot(weighted.T, flat, precision=lax.Precision.HIGHEST)
    counts = jnp.sum(weighted, axis=0)
    mine = jnp.take(sums, cluster_ids, axis=0).reshape(CLIENTS, HID, OUT)
    denom = jnp.take(counts, cluster_ids, axis=0)
    return mine / (LR * denom)[:, None, None]
```

```python
import functools

import jax
import jax.numpy as jnp
from jax import lax
from jax.experimental import pallas as pl
from jax.experimental.pallas import tpu as pltpu
from jax.sharding import PartitionSpec as P

LR = 0.5
CLUSTERS = 8
LANES = 128
TILE = 512
GRAD_ROWS = 256
SHARE = 8
LAG = 2
MESH = pl.DeviceIdType.MESH


def halves(value):
    high = value.astype(jnp.bfloat16)
    low = (value - high.astype(jnp.float32)).astype(jnp.bfloat16)
    return high, low


def dot(a, b):
    return jnp.dot(a, b, preferred_element_type=jnp.float32)


def round_kernel(
    sizes, x_hbm, lower_hbm, target_hbm, head_hbm, rows_hbm, count_ref, id_ref, out_ref,
    x_buf, lower, target, head, rows_ref, hid_hi, hid_lo, hid_t_hi, hid_t_lo, drawn, w_hi, w_lo, err_hi, err_lo, delta,
    facts, chosen, inbox, own, other, outbox, result,
    x_sem, in_sem, fact_send, fact_recv, share_send, share_recv, pair_send, pair_recv, back_send, back_recv,
):
    pool = x_buf.shape[0]
    tile = x_buf.shape[0] // x_sem.shape[0]
    tiles = pool // tile
    steps, count_rows = rows_ref.shape
    hid, width = head.shape
    chip_count, board_count, cuts_count = sizes
    plane = chip_count * cuts_count
    number = plane * board_count
    half = board_count // 2
    members = half * plane
    chunks = inbox.shape[0]
    block = hid // chunks
    share = block // plane

    chip, board, cuts = lax.axis_index("chip"), lax.axis_index("board"), lax.axis_index("cuts")
    seat = chip * cuts_count + cuts
    me = board * plane + seat
    side = (board >= half).astype(jnp.int32)
    hub = half - 1 + side
    is_hub = board == hub
    member = (board - side * half) * plane + seat

    def at(board_index, seat_index):
        return (lax.div(seat_index, cuts_count), board_index, lax.rem(seat_index, cuts_count))

    def x_copy(i):
        part = pl.ds(i * tile, tile)
        return pltpu.make_async_copy(x_hbm.at[0, part], x_buf.at[part], x_sem.at[i])

    rows_copy = pltpu.make_async_copy(rows_hbm.at[0], rows_ref, in_sem.at[0])
    lower_copy = pltpu.make_async_copy(lower_hbm.at[0], lower, in_sem.at[1])
    head_copy = pltpu.make_async_copy(head_hbm.at[0], head, in_sem.at[2])
    target_copy = pltpu.make_async_copy(target_hbm.at[0], target, in_sem.at[3])
    rows_copy.start()
    lower_copy.start()
    x_copy(0).start()
    head_copy.start()
    target_copy.start()
    for i in range(1, tiles):
        x_copy(i).start()

    barrier = pltpu.get_barrier_semaphore()

    def greet(offset, carry):
        peer = lax.rem(me + offset, number)
        pl.semaphore_signal(barrier, inc=1, device_id=at(lax.div(peer, plane), lax.rem(peer, plane)), device_id_type=MESH)
        return carry

    lax.fori_loop(1, number, greet, 0)
    kind = lax.broadcasted_iota(jnp.int32, (CLUSTERS, LANES), 0)
    facts[me] = jnp.where(kind == id_ref[0], count_ref[0].astype(jnp.float32), 0.0)

    rows_copy.wait()
    blocks = pool // LANES
    for step in range(steps):
        rows = rows_ref[step : step + 1, :]
        outer = lax.shift_right_logical(rows, 7)
        inner = lax.bitwise_and(rows, LANES - 1)
        one_outer = (lax.broadcasted_iota(jnp.int32, (blocks, count_rows), 0) == outer).astype(jnp.float32).astype(jnp.bfloat16)
        one_inner = (lax.broadcasted_iota(jnp.int32, (LANES, count_rows), 0) == inner).astype(jnp.float32).astype(jnp.bfloat16)
        table = lax.dot_general(one_inner, one_outer, (((1,), (1,)), ((), ())), preferred_element_type=jnp.float32)
        for j in range(blocks):
            drawn[step, j * LANES : (j + 1) * LANES, :] = jnp.broadcast_to(table[:, j : j + 1], (LANES, LANES))

    head_copy.wait()
    high, low = halves(head[...])
    w_hi[...] = high
    w_lo[...] = low
    lower_copy.wait()
    target_copy.wait()
    scale = -LR / count_rows

    def error(step, part, h_hi, h_lo):
        err = dot(h_hi, w_hi[...]) + dot(h_hi, w_lo[...]) + dot(h_lo, w_hi[...])
        err = err - target[part, :].astype(jnp.float32)
        err = err * jnp.concatenate([drawn[step, part, :]] * (width // LANES), axis=1) * scale
        e_hi, e_lo = halves(err)
        err_hi[part, :] = e_hi
        err_lo[part, :] = e_lo

    def gradient(part):
        return dot(hid_t_hi[part, :], err_hi[...]) + dot(hid_t_hi[part, :], err_lo[...]) + dot(hid_t_lo[part, :], err_hi[...])

    for i in range(tiles):
        part = pl.ds(i * tile, tile)
        x_copy(i).wait()
        h_hi, h_lo = halves(jnp.tanh(dot(x_buf[part, :], lower[...])))
        hid_hi[part, :] = h_hi
        hid_lo[part, :] = h_lo
        hid_t_hi[:, part] = h_hi.T
        hid_t_lo[:, part] = h_lo.T
        error(0, part, h_hi, h_lo)

    pl.semaphore_wait(barrier, number - 1)

    def tell(offset, carry):
        peer = lax.rem(seat + offset, plane)
        for where in (half - 1, half):
            @pl.when((offset > 0) | (board != where))
            def _():
                pltpu.make_async_remote_copy(
                    src_ref=facts.at[me], dst_ref=facts.at[me], send_sem=fact_send, recv_sem=fact_recv,
                    device_id=at(where, peer), device_id_type=MESH,
                ).start()
        return carry

    lax.fori_loop(0, plane, tell, 0)

    def rows_of(k, seat_index):
        return pl.ds(pl.multiple_of(k * block + seat_index * share, 8), share)

    def give_share(k, offset):
        peer = lax.rem(seat + offset, plane)
        pltpu.make_async_remote_copy(
            src_ref=delta.at[rows_of(k, peer)], dst_ref=inbox.at[k, member],
            send_sem=share_send, recv_sem=share_recv.at[k],
            device_id=at(hub, peer), device_id_type=MESH,
        ).start()

    grad_rows = min(GRAD_ROWS, hid)
    for step in range(steps):
        if step > 0:
            for i in range(tiles):
                part = pl.ds(i * tile, tile)
                error(step, part, hid_hi[part, :], hid_lo[part, :])
        for i in range(hid // grad_rows):
            part = pl.ds(i * grad_rows, grad_rows)
            value = gradient(part)
            if step > 0:
                value = value + delta[part, :]
            delta[part, :] = value
            if step + 1 < steps:
                high, low = halves(head[part, :] + value)
                w_hi[part, :] = high
                w_lo[part, :] = low
            else:
                for k in range(i * grad_rows // block, (i + 1) * grad_rows // block):
                    @pl.when(is_hub)
                    def _(k=k):
                        inbox[k, member] = delta[rows_of(k, seat), :]

                    @pl.when(jnp.logical_not(is_hub))
                    def _(k=k):
                        give_share(k, 0)

                    for offset in range(1, plane):
                        give_share(k, offset)

    def arrived(ref, sem):
        pltpu.make_async_copy(ref, ref, sem).wait()

    def wide(row):
        return jnp.concatenate([row] * (width // LANES), axis=1)

    def pair_copy(k):
        return pltpu.make_async_remote_copy(
            src_ref=own.at[k], dst_ref=other.at[k], send_sem=pair_send.at[k], recv_sem=pair_recv.at[k],
            device_id=at(board_count - 1 - hub, seat), device_id_type=MESH,
        )

    @pl.when(is_hub)
    def _():
        arrived(facts.at[pl.ds(0, number - 1)], fact_recv)
        counts = jnp.sum(facts[...], axis=0)
        inverse = 1.0 / (LR * jnp.maximum(counts, 1.0))
        first = side * members
        for t in range(members):
            chosen[t] = jnp.where(facts[first + t] > 0, inverse, 0.0)

        def add_up(k):
            arrived(inbox.at[k, pl.ds(0, members - 1)], share_recv.at[k])
            sums = [jnp.zeros((share, width), jnp.float32)] * CLUSTERS
            for t in range(members):
                value = inbox[k, t]
                for c in range(CLUSTERS):
                    sums[c] = sums[c] + wide(facts[first + t, c : c + 1, :]) * value
            for c in range(CLUSTERS):
                own[k, c] = sums[c]
            pair_copy(k).start()

        def give_back(k):
            arrived(other.at[k], pair_recv.at[k])
            total = [own[k, c] + other[k, c] for c in range(CLUSTERS)]
            for t in range(members):
                value = wide(chosen[t, 0:1, :]) * total[0]
                for c in range(1, CLUSTERS):
                    value = value + wide(chosen[t, c : c + 1, :]) * total[c]
                outbox[k, t] = value
            result[rows_of(k, seat), :] = outbox[k, member]

            def give(offset, carry):
                target_member = lax.rem(member + offset, members)
                pltpu.make_async_remote_copy(
                    src_ref=outbox.at[k, target_member], dst_ref=result.at[rows_of(k, seat)],
                    send_sem=back_send, recv_sem=back_recv,
                    device_id=at(side * half + lax.div(target_member, plane), lax.rem(target_member, plane)), device_id_type=MESH,
                ).start()
                return carry

            lax.fori_loop(1, members, give, 0)

        def tick(step, carry):
            @pl.when(step < chunks)
            def _():
                add_up(step)

            @pl.when(step >= LAG)
            def _():
                give_back(step - LAG)

            return carry

        lax.fori_loop(0, chunks + LAG, tick, 0)
        arrived(result.at[pl.ds(0, chunks * (plane - 1) * share)], back_recv)

    @pl.when(jnp.logical_not(is_hub))
    def _():
        arrived(result, back_recv)

    out_ref[0] = result[...]

    @pl.when(is_hub)
    def _():
        arrived(delta.at[pl.ds(0, chunks * (plane - 1) * share)], share_send)
        arrived(facts.at[pl.ds(0, 2 * plane - 1)], fact_send)
        for k in range(chunks):
            arrived(own.at[k], pair_send.at[k])
        arrived(outbox.at[:, pl.ds(0, members - 1)], back_send)

    @pl.when(jnp.logical_not(is_hub))
    def _():
        arrived(delta, share_send)
        arrived(facts.at[pl.ds(0, 2 * plane)], fact_send)


def federated_round(sizes, features, targets, lower_weight, head_weight, batch_rows, sample_counts, cluster_ids):
    pool, features_in = features.shape[1:]
    hid, width = head_weight.shape[1:]
    steps, count_rows = batch_rows.shape[1:]
    plane = sizes[0] * sizes[2]
    number = plane * sizes[1]
    members = number // 2
    share = SHARE
    chunks = hid // (plane * share)
    tiles = pool // min(TILE, pool)
    vmem = pl.BlockSpec(memory_space=pltpu.VMEM)
    smem = pl.BlockSpec(memory_space=pltpu.SMEM)
    hbm = pl.BlockSpec(memory_space=pltpu.HBM)
    half_type, full_type = jnp.bfloat16, jnp.float32
    one, many = pltpu.SemaphoreType.DMA, pltpu.SemaphoreType.DMA((chunks,))
    return pl.pallas_call(
        functools.partial(round_kernel, sizes),
        name="federated_round",
        out_shape=jax.ShapeDtypeStruct((1, hid, width), full_type),
        in_specs=[hbm] * 5 + [smem] * 2,
        out_specs=vmem,
        scratch_shapes=[
            pltpu.VMEM((pool, features_in), half_type),
            pltpu.VMEM((features_in, hid), half_type),
            pltpu.VMEM((pool, width), half_type),
            pltpu.VMEM((hid, width), full_type),
            pltpu.VMEM((steps, count_rows), jnp.int32),
            pltpu.VMEM((pool, hid), half_type),
            pltpu.VMEM((pool, hid), half_type),
            pltpu.VMEM((hid, pool), half_type),
            pltpu.VMEM((hid, pool), half_type),
            pltpu.VMEM((steps, pool, LANES), full_type),
            pltpu.VMEM((hid, width), half_type),
            pltpu.VMEM((hid, width), half_type),
            pltpu.VMEM((pool, width), half_type),
            pltpu.VMEM((pool, width), half_type),
            pltpu.VMEM((hid, width), full_type),
            pltpu.VMEM((number, CLUSTERS, LANES), full_type),
            pltpu.VMEM((members, CLUSTERS, LANES), full_type),
            pltpu.VMEM((chunks, members, share, width), full_type),
            pltpu.VMEM((chunks, CLUSTERS, share, width), full_type),
            pltpu.VMEM((chunks, CLUSTERS, share, width), full_type),
            pltpu.VMEM((chunks, members, share, width), full_type),
            pltpu.VMEM((hid, width), full_type),
            pltpu.SemaphoreType.DMA((tiles,)),
            pltpu.SemaphoreType.DMA((4,)),
            one, one, one, many, many, many, one, one,
        ],
        compiler_params=pltpu.CompilerParams(collective_id=0, has_side_effects=True, vmem_limit_bytes=56 * 2**20),
    )(features, lower_weight, targets, head_weight, batch_rows, sample_counts, cluster_ids)


def solution(mesh):
    sizes = (mesh.shape["chip"], mesh.shape["board"], mesh.shape["cuts"])
    rows, flat = P(("chip", "board", "cuts"), None, None), P(("chip", "board", "cuts"))
    return jax.shard_map(
        functools.partial(federated_round, sizes),
        mesh=mesh,
        in_specs=(rows, rows, rows, rows, rows, flat, flat),
        out_specs=rows,
        check_vma=False,
    )
```

```python
import functools

import jax
import jax.numpy as jnp
from jax import lax
from jax.experimental import pallas as pl
from jax.experimental.pallas import tpu as pltpu
from jax.sharding import PartitionSpec as P

LR = 0.5
CLUSTERS = 8
LANES = 128
TILE = 512
GRAD_ROWS = 256
SHARE = 8
COLUMNS = 128
LAG = 4
LIMIT = 53
WAIT = 1
MESH = pl.DeviceIdType.MESH


def halves(value):
    high = value.astype(jnp.bfloat16)
    low = (value - high.astype(jnp.float32)).astype(jnp.bfloat16)
    return high, low


def dot(a, b):
    return jnp.dot(a, b, preferred_element_type=jnp.float32)


def round_kernel(
    sizes, x_hbm, lower_hbm, target_hbm, head_hbm, rows_hbm, count_ref, id_ref, out_ref,
    x_buf, lower, target, head, rows_ref, hid_hi, hid_lo, hid_t_hi, hid_t_lo, drawn, w_hi, w_lo, err_hi, err_lo, delta,
    facts, chosen, inbox, own, other, outbox, result,
    x_sem, in_sem, fact_send, fact_recv, share_send, share_recv, pair_send, pair_recv, back_send, back_recv,
):
    pool = x_buf.shape[0]
    tile = x_buf.shape[0] // x_sem.shape[0]
    tiles = pool // tile
    steps, count_rows = rows_ref.shape
    hid, width = head.shape
    chip_count, board_count, cuts_count = sizes
    plane = chip_count * cuts_count
    number = plane * board_count
    half = board_count // 2
    members = half * plane
    chunks, _, share, columns = inbox.shape
    groups = width // columns
    block = plane * share

    chip, board, cuts = lax.axis_index("chip"), lax.axis_index("board"), lax.axis_index("cuts")
    seat = chip * cuts_count + cuts
    me = board * plane + seat
    side = (board >= half).astype(jnp.int32)
    hub = half - 1 + side
    is_hub = board == hub
    hub_row = (half - 1) * (1 - side)
    row = board - side * half
    member = row * plane + seat

    def toggled(value, mask):
        return value if mask == 0 else lax.bitwise_xor(value, mask)

    def far_first(masks):
        order = sorted(masks, key=lambda mask: -bin(mask).count("1"))
        across = [mask for mask in order if mask % cuts_count > 1]
        rest = [mask for mask in order if mask % cuts_count <= 1]
        mixed = []
        while across or rest:
            mixed += across[:1] + rest[:1]
            across, rest = across[1:], rest[1:]
        return mixed

    def seat_of(mask):
        c, k = toggled(chip, mask // cuts_count), toggled(cuts, mask % cuts_count)
        return c, k, c * cuts_count + k

    def everyone(boards, act):
        def on_board(i, carry):
            where = boards + i
            for c in range(chip_count):
                for k in range(cuts_count):
                    @pl.when((where != board) | (chip != c) | (cuts != k))
                    def _(c=c, k=k):
                        act((c, where, k))

            return carry

        return lambda count: lax.fori_loop(0, count, on_board, 0)

    def x_copy(i):
        part = pl.ds(i * tile, tile)
        return pltpu.make_async_copy(x_hbm.at[0, part], x_buf.at[part], x_sem.at[i])

    rows_copy = pltpu.make_async_copy(rows_hbm.at[0], rows_ref, in_sem.at[0])
    lower_copy = pltpu.make_async_copy(lower_hbm.at[0], lower, in_sem.at[1])
    head_copy = pltpu.make_async_copy(head_hbm.at[0], head, in_sem.at[2])
    target_copy = pltpu.make_async_copy(target_hbm.at[0], target, in_sem.at[3])
    rows_copy.start()
    lower_copy.start()
    x_copy(0).start()
    head_copy.start()
    target_copy.start()
    for i in range(1, tiles):
        x_copy(i).start()

    barrier = pltpu.get_barrier_semaphore()

    everyone(0, lambda device: pl.semaphore_signal(barrier, inc=1, device_id=device, device_id_type=MESH))(board_count)
    kind = lax.broadcasted_iota(jnp.int32, (CLUSTERS, LANES), 0)
    facts[me] = jnp.where(kind == id_ref[0], count_ref[0].astype(jnp.float32), 0.0)

    rows_copy.wait()
    blocks = pool // LANES
    for step in range(steps):
        rows = rows_ref[step : step + 1, :]
        outer = lax.shift_right_logical(rows, 7)
        inner = lax.bitwise_and(rows, LANES - 1)
        one_outer = (lax.broadcasted_iota(jnp.int32, (blocks, count_rows), 0) == outer).astype(jnp.float32).astype(jnp.bfloat16)
        one_inner = (lax.broadcasted_iota(jnp.int32, (LANES, count_rows), 0) == inner).astype(jnp.float32).astype(jnp.bfloat16)
        table = lax.dot_general(one_inner, one_outer, (((1,), (1,)), ((), ())), preferred_element_type=jnp.float32)
        for j in range(blocks):
            drawn[step, j * LANES : (j + 1) * LANES, :] = jnp.broadcast_to(table[:, j : j + 1], (LANES, LANES))

    head_copy.wait()
    high, low = halves(head[...])
    w_hi[...] = high
    w_lo[...] = low
    lower_copy.wait()
    scale = -LR / count_rows

    def error(step, part, h_hi, h_lo):
        err = dot(h_hi, w_hi[...]) + dot(h_hi, w_lo[...]) + dot(h_lo, w_hi[...])
        err = err - target[part, :].astype(jnp.float32)
        err = err * jnp.concatenate([drawn[step, part, :]] * (width // LANES), axis=1) * scale
        e_hi, e_lo = halves(err)
        err_hi[part, :] = e_hi
        err_lo[part, :] = e_lo

    def gradient(part):
        return dot(hid_t_hi[part, :], err_hi[...]) + dot(hid_t_hi[part, :], err_lo[...]) + dot(hid_t_lo[part, :], err_hi[...])

    def keep(part, product):
        h_hi, h_lo = halves(jnp.tanh(product))
        hid_hi[part, :] = h_hi
        hid_lo[part, :] = h_lo
        hid_t_hi[:, part] = h_hi.T
        hid_t_lo[:, part] = h_lo.T
        return h_hi, h_lo

    parts = [pl.ds(i * tile, tile) for i in range(tiles)]
    for i in range(WAIT):
        x_copy(i).wait()
    kept = None
    for i in range(tiles):
        if i == WAIT:
            for k in range(WAIT, tiles):
                x_copy(k).wait()
            target_copy.wait()
        product = dot(x_buf[parts[i], :], lower[...])
        if kept is not None:
            error(0, parts[i - 1], *kept)
        kept = keep(parts[i], product)
    if WAIT >= tiles:
        target_copy.wait()
    error(0, parts[-1], *kept)

    pl.semaphore_wait(barrier, number - 1)

    def tell(device):
        pltpu.make_async_remote_copy(
            src_ref=facts.at[me], dst_ref=facts.at[me], send_sem=fact_send, recv_sem=fact_recv,
            device_id=device, device_id_type=MESH,
        ).start()

    everyone(half - 1, tell)(2)

    def rows_of(k, seat_index):
        return pl.ds(pl.multiple_of(lax.div(k, groups) * block + seat_index * share, 8), share)

    def columns_of(k):
        return pl.ds(pl.multiple_of(lax.rem(k, groups) * columns, LANES), columns)

    def give_share(k, mask):
        c, z, peer = seat_of(mask)
        pltpu.make_async_remote_copy(
            src_ref=delta.at[rows_of(k, peer), columns_of(k)], dst_ref=inbox.at[k, member],
            send_sem=share_send, recv_sem=share_recv.at[k],
            device_id=(c, hub, z), device_id_type=MESH,
        ).start()

    def give_shares(k):
        @pl.when(is_hub)
        def _():
            inbox[k, member] = delta[rows_of(k, seat), columns_of(k)]

        for mask in far_first(range(plane)):
            if mask > 0:
                give_share(k, mask)
            else:
                @pl.when(jnp.logical_not(is_hub))
                def _():
                    give_share(k, 0)

    grad_rows = min(GRAD_ROWS, hid)
    for step in range(steps):
        if step > 0:
            for i in range(tiles):
                part = pl.ds(i * tile, tile)
                error(step, part, hid_hi[part, :], hid_lo[part, :])
        for i in range(hid // grad_rows):
            part = pl.ds(i * grad_rows, grad_rows)
            value = gradient(part)
            if step > 0:
                value = value + delta[part, :]
            delta[part, :] = value
            if step + 1 < steps:
                high, low = halves(head[part, :] + value)
                w_hi[part, :] = high
                w_lo[part, :] = low
            else:
                def send(k, carry):
                    give_shares(k)
                    return carry

                per_row = groups * grad_rows // block
                lax.fori_loop(i * per_row, (i + 1) * per_row, send, 0)

    def arrived(ref, sem):
        pltpu.make_async_copy(ref, ref, sem).wait()

    moved = pl.ds(0, hid // plane * (plane - 1))

    def wide(line):
        return line if columns == LANES else jnp.concatenate([line] * (columns // LANES), axis=1)

    def pair_copy(k):
        return pltpu.make_async_remote_copy(
            src_ref=own.at[k], dst_ref=other.at[k], send_sem=pair_send.at[k], recv_sem=pair_recv.at[k],
            device_id=(chip, board_count - 1 - hub, cuts), device_id_type=MESH,
        )

    @pl.when(is_hub)
    def _():
        arrived(facts.at[pl.ds(0, number - 1)], fact_recv)
        counts = jnp.sum(facts[...], axis=0)
        inverse = 1.0 / (LR * jnp.maximum(counts, 1.0))
        first = side * members
        for t in range(members):
            chosen[t] = jnp.where(facts[first + t] > 0, inverse, 0.0)

        def add_up(k):
            arrived(inbox.at[k, pl.ds(0, members - 1)], share_recv.at[k])
            sums = [jnp.zeros((share, columns), jnp.float32)] * CLUSTERS
            for t in range(members):
                value = inbox[k, t]
                for c in range(CLUSTERS):
                    sums[c] = sums[c] + wide(facts[first + t, c : c + 1, :]) * value
            for c in range(CLUSTERS):
                own[k, c] = sums[c]
            pair_copy(k).start()

        def give_back(k):
            arrived(other.at[k], pair_recv.at[k])
            total = [own[k, c] + other[k, c] for c in range(CLUSTERS)]
            for t in range(members):
                value = wide(chosen[t, 0:1, :]) * total[0]
                for c in range(1, CLUSTERS):
                    value = value + wide(chosen[t, c : c + 1, :]) * total[c]
                outbox[k, t] = value
            result[rows_of(k, seat), columns_of(k)] = outbox[k, member]
            for mask in far_first(range(1, members)):
                c, z, peer = seat_of(mask % plane)
                peer_row = toggled(hub_row, mask // plane)
                pltpu.make_async_remote_copy(
                    src_ref=outbox.at[k, peer_row * plane + peer], dst_ref=result.at[rows_of(k, seat), columns_of(k)],
                    send_sem=back_send, recv_sem=back_recv,
                    device_id=(c, side * half + peer_row, z), device_id_type=MESH,
                ).start()

        lag = min(LAG, chunks)

        def first_ticks(k, carry):
            add_up(k)
            return carry

        def ticks(k, carry):
            add_up(k)
            give_back(k - lag)
            return carry

        def last_ticks(k, carry):
            give_back(k)
            return carry

        lax.fori_loop(0, lag, first_ticks, 0)
        lax.fori_loop(lag, chunks, ticks, 0)
        lax.fori_loop(chunks - lag, chunks, last_ticks, 0)
        arrived(result.at[moved], back_recv)

    @pl.when(jnp.logical_not(is_hub))
    def _():
        arrived(result, back_recv)

    out_ref[0] = result[...]

    @pl.when(is_hub)
    def _():
        arrived(delta.at[moved], share_send)
        arrived(facts.at[pl.ds(0, 2 * plane - 1)], fact_send)
        for k in range(chunks):
            arrived(own.at[k], pair_send.at[k])
        arrived(outbox.at[:, pl.ds(0, members - 1)], back_send)

    @pl.when(jnp.logical_not(is_hub))
    def _():
        arrived(delta, share_send)
        arrived(facts.at[pl.ds(0, 2 * plane)], fact_send)


def federated_round(sizes, features, targets, lower_weight, head_weight, batch_rows, sample_counts, cluster_ids):
    pool, features_in = features.shape[1:]
    hid, width = head_weight.shape[1:]
    steps, count_rows = batch_rows.shape[1:]
    plane = sizes[0] * sizes[2]
    number = plane * sizes[1]
    members = number // 2
    share = SHARE
    columns = COLUMNS
    chunks = hid // (plane * share) * (width // columns)
    tiles = pool // min(TILE, pool)
    vmem = pl.BlockSpec(memory_space=pltpu.VMEM)
    smem = pl.BlockSpec(memory_space=pltpu.SMEM)
    hbm = pl.BlockSpec(memory_space=pltpu.HBM)
    half_type, full_type = jnp.bfloat16, jnp.float32
    one, many = pltpu.SemaphoreType.DMA, pltpu.SemaphoreType.DMA((chunks,))
    return pl.pallas_call(
        functools.partial(round_kernel, sizes),
        name="federated_round",
        out_shape=jax.ShapeDtypeStruct((1, hid, width), full_type),
        in_specs=[hbm] * 5 + [smem] * 2,
        out_specs=vmem,
        scratch_shapes=[
            pltpu.VMEM((pool, features_in), half_type),
            pltpu.VMEM((features_in, hid), half_type),
            pltpu.VMEM((pool, width), half_type),
            pltpu.VMEM((hid, width), full_type),
            pltpu.VMEM((steps, count_rows), jnp.int32),
            pltpu.VMEM((pool, hid), half_type),
            pltpu.VMEM((pool, hid), half_type),
            pltpu.VMEM((hid, pool), half_type),
            pltpu.VMEM((hid, pool), half_type),
            pltpu.VMEM((steps, pool, LANES), full_type),
            pltpu.VMEM((hid, width), half_type),
            pltpu.VMEM((hid, width), half_type),
            pltpu.VMEM((pool, width), half_type),
            pltpu.VMEM((pool, width), half_type),
            pltpu.VMEM((hid, width), full_type),
            pltpu.VMEM((number, CLUSTERS, LANES), full_type),
            pltpu.VMEM((members, CLUSTERS, LANES), full_type),
            pltpu.VMEM((chunks, members, share, columns), full_type),
            pltpu.VMEM((chunks, CLUSTERS, share, columns), full_type),
            pltpu.VMEM((chunks, CLUSTERS, share, columns), full_type),
            pltpu.VMEM((chunks, members, share, columns), full_type),
            pltpu.VMEM((hid, width), full_type),
            pltpu.SemaphoreType.DMA((tiles,)),
            pltpu.SemaphoreType.DMA((4,)),
            one, one, one, many, many, many, one, one,
        ],
        compiler_params=pltpu.CompilerParams(collective_id=0, has_side_effects=True, vmem_limit_bytes=LIMIT * 2**20),
    )(features, lower_weight, targets, head_weight, batch_rows, sample_counts, cluster_ids)


def solution(mesh):
    sizes = (mesh.shape["chip"], mesh.shape["board"], mesh.shape["cuts"])
    rows, flat = P(("chip", "board", "cuts"), None, None), P(("chip", "board", "cuts"))
    return jax.shard_map(
        functools.partial(federated_round, sizes),
        mesh=mesh,
        in_specs=(rows, rows, rows, rows, rows, flat, flat),
        out_specs=rows,
        check_vma=False,
    )
```

```python
import functools

import jax
import jax.numpy as jnp
from jax import lax
from jax.experimental import pallas as pl
from jax.experimental.pallas import tpu as pltpu
from jax.sharding import PartitionSpec as P

LR = 0.5
CLUSTERS = 8
LANES = 128
TILE = 512
GRAD_ROWS = 256
SHARE = 8
COLUMNS = 128
LAG = 6
LIMIT = 53
WAIT = 2
MESH = pl.DeviceIdType.MESH


def halves(value):
    high = value.astype(jnp.bfloat16)
    low = (value - high.astype(jnp.float32)).astype(jnp.bfloat16)
    return high, low


def dot(a, b):
    return jnp.dot(a, b, preferred_element_type=jnp.float32)


def round_kernel(
    sizes, x_hbm, lower_hbm, target_hbm, head_hbm, rows_hbm, count_ref, id_ref, out_ref,
    x_buf, lower, target, head, rows_ref, hid_hi, hid_lo, hid_t_hi, hid_t_lo, drawn, w_first, w_pack, low_rest, err_pack, delta,
    facts, chosen, inbox, own, other, outbox, result,
    x_sem, in_sem, fact_send, fact_recv, share_send, share_recv, pair_send, pair_recv, back_send, back_recv,
):
    pool = x_buf.shape[0]
    tile = x_buf.shape[0] // x_sem.shape[0]
    tiles = pool // tile
    steps, count_rows = rows_ref.shape
    hid, width = head.shape
    chip_count, board_count, cuts_count = sizes
    plane = chip_count * cuts_count
    number = plane * board_count
    half = board_count // 2
    members = half * plane
    chunks, _, share, columns = inbox.shape
    groups = width // columns
    block = plane * share

    chip, board, cuts = lax.axis_index("chip"), lax.axis_index("board"), lax.axis_index("cuts")
    seat = chip * cuts_count + cuts
    me = board * plane + seat
    side = (board >= half).astype(jnp.int32)
    hub = half - 1 + side
    is_hub = board == hub
    hub_row = (half - 1) * (1 - side)
    row = board - side * half
    member = row * plane + seat

    def toggled(value, mask):
        return value if mask == 0 else lax.bitwise_xor(value, mask)

    def far_first(masks):
        order = sorted(masks, key=lambda mask: -bin(mask).count("1"))
        across = [mask for mask in order if mask % cuts_count > 1]
        rest = [mask for mask in order if mask % cuts_count <= 1]
        mixed = []
        while across or rest:
            mixed += across[:1] + rest[:1]
            across, rest = across[1:], rest[1:]
        return mixed

    def seat_of(mask):
        c, k = toggled(chip, mask // cuts_count), toggled(cuts, mask % cuts_count)
        return c, k, c * cuts_count + k

    def everyone(boards, act):
        def on_board(i, carry):
            where = boards + i
            for c in range(chip_count):
                for k in range(cuts_count):
                    @pl.when((where != board) | (chip != c) | (cuts != k))
                    def _(c=c, k=k):
                        act((c, where, k))

            return carry

        return lambda count: lax.fori_loop(0, count, on_board, 0)

    def x_copy(i):
        part = pl.ds(i * tile, tile)
        return pltpu.make_async_copy(x_hbm.at[0, part], x_buf.at[part], x_sem.at[i])

    rows_copy = pltpu.make_async_copy(rows_hbm.at[0], rows_ref, in_sem.at[0])
    lower_copy = pltpu.make_async_copy(lower_hbm.at[0], lower, in_sem.at[1])
    head_copy = pltpu.make_async_copy(head_hbm.at[0], head, in_sem.at[2])
    target_copy = pltpu.make_async_copy(target_hbm.at[0], target, in_sem.at[3])
    rows_copy.start()
    lower_copy.start()
    x_copy(0).start()
    head_copy.start()
    target_copy.start()
    for i in range(1, tiles):
        x_copy(i).start()

    barrier = pltpu.get_barrier_semaphore()

    everyone(0, lambda device: pl.semaphore_signal(barrier, inc=1, device_id=device, device_id_type=MESH))(board_count)
    kind = lax.broadcasted_iota(jnp.int32, (CLUSTERS, LANES), 0)
    facts[me] = jnp.where(kind == id_ref[0], count_ref[0].astype(jnp.float32), 0.0)

    rows_copy.wait()
    blocks = pool // LANES
    for step in range(steps):
        rows = rows_ref[step : step + 1, :]
        outer = lax.shift_right_logical(rows, 7)
        inner = lax.bitwise_and(rows, LANES - 1)
        one_outer = (lax.broadcasted_iota(jnp.int32, (blocks, count_rows), 0) == outer).astype(jnp.float32).astype(jnp.bfloat16)
        one_inner = (lax.broadcasted_iota(jnp.int32, (LANES, count_rows), 0) == inner).astype(jnp.float32).astype(jnp.bfloat16)
        table = lax.dot_general(one_inner, one_outer, (((1,), (1,)), ((), ())), preferred_element_type=jnp.float32)
        for j in range(blocks):
            drawn[step, j * LANES : (j + 1) * LANES, :] = jnp.broadcast_to(table[:, j : j + 1], (LANES, LANES))

    head_copy.wait()
    def wide(line):
        return line if columns == LANES else jnp.concatenate([line] * (columns // LANES), axis=1)

    def lanes(j):
        return pl.ds(j * columns, columns)

    here, rest = pl.ds(0, columns), pl.ds(columns, columns)
    for j in range(groups):
        high, low = halves(head[:, lanes(j)])
        w_first[:, lanes(j)] = high
        w_pack[j, :, here] = high
        w_pack[j, :, rest] = low
    lower_copy.wait()
    scale = -LR / count_rows

    def error(step, j, part, h_hi, low_term):
        both = dot(h_hi, w_pack[j])
        err = both[:, :columns] + both[:, columns:] + low_term
        err = err - target[part, lanes(j)].astype(jnp.float32)
        err = err * wide(drawn[step, part, :]) * scale
        e_hi, e_lo = halves(err)
        err_pack[part, here] = e_hi
        err_pack[part, rest] = e_lo

    def first_error(part, h_hi, h_lo):
        low = dot(h_lo, w_first[...])
        for j in range(1, groups):
            low_rest[j - 1, part, :] = low[:, j * columns : (j + 1) * columns]
        error(0, 0, part, h_hi, low[:, :columns])

    def gradient(part):
        both = dot(hid_t_hi[part, :], err_pack[...])
        return both[:, :columns] + both[:, columns:] + dot(hid_t_lo[part, :], err_pack[:, here])

    def keep(part, product):
        h_hi, h_lo = halves(jnp.tanh(product))
        hid_hi[part, :] = h_hi
        hid_lo[part, :] = h_lo
        hid_t_hi[:, part] = h_hi.T
        hid_t_lo[:, part] = h_lo.T
        return h_hi, h_lo

    parts = [pl.ds(i * tile, tile) for i in range(tiles)]
    for i in range(min(WAIT, tiles)):
        x_copy(i).wait()
    kept = None
    for i in range(tiles):
        if i == WAIT:
            for k in range(WAIT, tiles):
                x_copy(k).wait()
        if i == 1:
            target_copy.wait()
        product = dot(x_buf[parts[i], :], lower[...])
        if kept is not None:
            first_error(parts[i - 1], *kept)
        kept = keep(parts[i], product)
    if tiles == 1:
        target_copy.wait()
    first_error(parts[-1], *kept)

    pl.semaphore_wait(barrier, number - 1)

    def tell(device):
        pltpu.make_async_remote_copy(
            src_ref=facts.at[me], dst_ref=facts.at[me], send_sem=fact_send, recv_sem=fact_recv,
            device_id=device, device_id_type=MESH,
        ).start()

    everyone(half - 1, tell)(2)

    def rows_of(k, seat_index):
        return pl.ds(pl.multiple_of(lax.rem(k, chunks // groups) * block + seat_index * share, 8), share)

    def group_of(k):
        return lax.div(k, chunks // groups)

    def columns_of(k):
        return pl.ds(pl.multiple_of(group_of(k) * columns, LANES), columns)

    def give_share(k, mask):
        c, z, peer = seat_of(mask)
        pltpu.make_async_remote_copy(
            src_ref=delta.at[group_of(k), rows_of(k, peer)], dst_ref=inbox.at[k, member],
            send_sem=share_send, recv_sem=share_recv.at[k],
            device_id=(c, hub, z), device_id_type=MESH,
        ).start()

    def give_shares(k):
        @pl.when(is_hub)
        def _():
            inbox[k, member] = delta[group_of(k), rows_of(k, seat), :]

        for mask in far_first(range(plane)):
            if mask > 0:
                give_share(k, mask)
            else:
                @pl.when(jnp.logical_not(is_hub))
                def _():
                    give_share(k, 0)

    grad_rows = min(GRAD_ROWS, hid)
    row_blocks = chunks // groups
    for j in range(groups):
        for step in range(steps):
            for part in parts:
                if step > 0:
                    error(step, j, part, hid_hi[part, :], dot(hid_lo[part, :], w_pack[j, :, here]))
                elif j > 0:
                    error(step, j, part, hid_hi[part, :], low_rest[j - 1, part, :])
            for i in range(hid // grad_rows):
                part = pl.ds(i * grad_rows, grad_rows)
                value = gradient(part)
                if step > 0:
                    value = value + delta[j, part, :]
                delta[j, part, :] = value
                if step + 1 < steps:
                    high, low = halves(head[part, lanes(j)] + value)
                    w_pack[j, part, here] = high
                    w_pack[j, part, rest] = low
                else:
                    def send(k, carry):
                        give_shares(k)
                        return carry

                    start = j * row_blocks + i * grad_rows // block
                    lax.fori_loop(start, start + grad_rows // block, send, 0)

    def arrived(ref, sem):
        pltpu.make_async_copy(ref, ref, sem).wait()

    moved = pl.ds(0, hid // plane * (plane - 1))

    def pair_copy(k):
        return pltpu.make_async_remote_copy(
            src_ref=own.at[k], dst_ref=other.at[k], send_sem=pair_send.at[k], recv_sem=pair_recv.at[k],
            device_id=(chip, board_count - 1 - hub, cuts), device_id_type=MESH,
        )

    @pl.when(is_hub)
    def _():
        arrived(facts.at[pl.ds(0, number - 1)], fact_recv)
        counts = jnp.sum(facts[...], axis=0)
        inverse = 1.0 / (LR * jnp.maximum(counts, 1.0))
        first = side * members
        for t in range(members):
            chosen[t] = jnp.where(facts[first + t] > 0, inverse, 0.0)

        def add_up(k):
            arrived(inbox.at[k, pl.ds(0, members - 1)], share_recv.at[k])
            sums = [jnp.zeros((share, columns), jnp.float32)] * CLUSTERS
            for t in range(members):
                value = inbox[k, t]
                for c in range(CLUSTERS):
                    sums[c] = sums[c] + wide(facts[first + t, c : c + 1, :]) * value
            for c in range(CLUSTERS):
                own[k, c] = sums[c]
            pair_copy(k).start()

        def give_back(k):
            arrived(other.at[k], pair_recv.at[k])
            total = [own[k, c] + other[k, c] for c in range(CLUSTERS)]
            for t in range(members):
                value = wide(chosen[t, 0:1, :]) * total[0]
                for c in range(1, CLUSTERS):
                    value = value + wide(chosen[t, c : c + 1, :]) * total[c]
                outbox[k, t] = value
            result[rows_of(k, seat), columns_of(k)] = outbox[k, member]
            for mask in far_first(range(1, members)):
                c, z, peer = seat_of(mask % plane)
                peer_row = toggled(hub_row, mask // plane)
                pltpu.make_async_remote_copy(
                    src_ref=outbox.at[k, peer_row * plane + peer], dst_ref=result.at[rows_of(k, seat), columns_of(k)],
                    send_sem=back_send, recv_sem=back_recv,
                    device_id=(c, side * half + peer_row, z), device_id_type=MESH,
                ).start()

        lag = min(LAG, chunks)

        def first_ticks(k, carry):
            add_up(k)
            return carry

        def ticks(k, carry):
            add_up(k)
            give_back(k - lag)
            return carry

        def last_ticks(k, carry):
            give_back(k)
            return carry

        lax.fori_loop(0, lag, first_ticks, 0)
        lax.fori_loop(lag, chunks, ticks, 0)
        lax.fori_loop(chunks - lag, chunks, last_ticks, 0)
        arrived(result.at[moved], back_recv)

    @pl.when(jnp.logical_not(is_hub))
    def _():
        arrived(result, back_recv)

    out_ref[0] = result[...]

    @pl.when(is_hub)
    def _():
        arrived(delta.at[:, moved], share_send)
        arrived(facts.at[pl.ds(0, 2 * plane - 1)], fact_send)
        for k in range(chunks):
            arrived(own.at[k], pair_send.at[k])
        arrived(outbox.at[:, pl.ds(0, members - 1)], back_send)

    @pl.when(jnp.logical_not(is_hub))
    def _():
        arrived(delta, share_send)
        arrived(facts.at[pl.ds(0, 2 * plane)], fact_send)


def federated_round(sizes, features, targets, lower_weight, head_weight, batch_rows, sample_counts, cluster_ids):
    pool, features_in = features.shape[1:]
    hid, width = head_weight.shape[1:]
    steps, count_rows = batch_rows.shape[1:]
    plane = sizes[0] * sizes[2]
    number = plane * sizes[1]
    members = number // 2
    share = SHARE
    columns = min(COLUMNS, width)
    groups = width // columns
    chunks = hid // (plane * share) * (width // columns)
    tiles = pool // min(TILE, pool)
    vmem = pl.BlockSpec(memory_space=pltpu.VMEM)
    smem = pl.BlockSpec(memory_space=pltpu.SMEM)
    hbm = pl.BlockSpec(memory_space=pltpu.HBM)
    half_type, full_type = jnp.bfloat16, jnp.float32
    one, many = pltpu.SemaphoreType.DMA, pltpu.SemaphoreType.DMA((chunks,))
    return pl.pallas_call(
        functools.partial(round_kernel, sizes),
        name="federated_round",
        out_shape=jax.ShapeDtypeStruct((1, hid, width), full_type),
        in_specs=[hbm] * 5 + [smem] * 2,
        out_specs=vmem,
        scratch_shapes=[
            pltpu.VMEM((pool, features_in), half_type),
            pltpu.VMEM((features_in, hid), half_type),
            pltpu.VMEM((pool, width), half_type),
            pltpu.VMEM((hid, width), full_type),
            pltpu.VMEM((steps, count_rows), jnp.int32),
            pltpu.VMEM((pool, hid), half_type),
            pltpu.VMEM((pool, hid), half_type),
            pltpu.VMEM((hid, pool), half_type),
            pltpu.VMEM((hid, pool), half_type),
            pltpu.VMEM((steps, pool, LANES), full_type),
            pltpu.VMEM((hid, width), half_type),
            pltpu.VMEM((groups, hid, 2 * columns), half_type),
            pltpu.VMEM((max(1, groups - 1), pool, columns), full_type),
            pltpu.VMEM((pool, 2 * columns), half_type),
            pltpu.VMEM((groups, hid, columns), full_type),
            pltpu.VMEM((number, CLUSTERS, LANES), full_type),
            pltpu.VMEM((members, CLUSTERS, LANES), full_type),
            pltpu.VMEM((chunks, members, share, columns), full_type),
            pltpu.VMEM((chunks, CLUSTERS, share, columns), full_type),
            pltpu.VMEM((chunks, CLUSTERS, share, columns), full_type),
            pltpu.VMEM((chunks, members, share, columns), full_type),
            pltpu.VMEM((hid, width), full_type),
            pltpu.SemaphoreType.DMA((tiles,)),
            pltpu.SemaphoreType.DMA((4,)),
            one, one, one, many, many, many, one, one,
        ],
        compiler_params=pltpu.CompilerParams(collective_id=0, has_side_effects=True, vmem_limit_bytes=LIMIT * 2**20),
    )(features, lower_weight, targets, head_weight, batch_rows, sample_counts, cluster_ids)


def solution(mesh):
    sizes = (mesh.shape["chip"], mesh.shape["board"], mesh.shape["cuts"])
    rows, flat = P(("chip", "board", "cuts"), None, None), P(("chip", "board", "cuts"))
    return jax.shard_map(
        functools.partial(federated_round, sizes),
        mesh=mesh,
        in_specs=(rows, rows, rows, rows, rows, flat, flat),
        out_specs=rows,
        check_vma=False,
    )
```

```python
import functools

import jax
import jax.numpy as jnp
from jax import lax
from jax.experimental import pallas as pl
from jax.experimental.pallas import tpu as pltpu
from jax.sharding import PartitionSpec as P

LR = 0.5
CLUSTERS = 8
LANES = 128
TILE = 512
GRAD_ROWS = 256
SHARE = 16
COLUMNS = 128
LAG = 2
LIMIT = 53
WAIT = 2
MESH = pl.DeviceIdType.MESH


def halves(value):
    high = value.astype(jnp.bfloat16)
    low = (value - high.astype(jnp.float32)).astype(jnp.bfloat16)
    return high, low


def dot(a, b):
    return jnp.dot(a, b, preferred_element_type=jnp.float32)


def round_kernel(
    sizes, x_hbm, lower_hbm, target_hbm, head_hbm, rows_hbm, count_ref, id_ref, out_ref,
    x_buf, lower, target, head, rows_ref, hid_hi, hid_lo, hid_t_hi, hid_t_lo, drawn, w_first, w_pack, low_rest, err_pack, delta,
    facts, chosen, inbox, own, other, outbox,
    x_sem, in_sem, fact_send, fact_recv, share_send, share_recv, pair_send, pair_recv, back_send, back_recv,
):
    pool = x_buf.shape[0]
    tile = x_buf.shape[0] // x_sem.shape[0]
    tiles = pool // tile
    steps, count_rows = rows_ref.shape
    hid, width = head.shape
    chip_count, board_count, cuts_count = sizes
    plane = chip_count * cuts_count
    number = plane * board_count
    half = board_count // 2
    members = half * plane
    chunks, _, share, columns = inbox.shape
    groups = width // columns
    block = plane * share

    chip, board, cuts = lax.axis_index("chip"), lax.axis_index("board"), lax.axis_index("cuts")
    seat = chip * cuts_count + cuts
    me = board * plane + seat
    side = (board >= half).astype(jnp.int32)
    hub = half - 1 + side
    is_hub = board == hub
    hub_row = (half - 1) * (1 - side)
    row = board - side * half
    member = row * plane + seat

    def toggled(value, mask):
        return value if mask == 0 else lax.bitwise_xor(value, mask)

    def far_first(masks):
        order = sorted(masks, key=lambda mask: -bin(mask).count("1"))
        across = [mask for mask in order if mask % cuts_count > 1]
        rest = [mask for mask in order if mask % cuts_count <= 1]
        mixed = []
        while across or rest:
            mixed += across[:1] + rest[:1]
            across, rest = across[1:], rest[1:]
        return mixed

    def seat_of(mask):
        c, k = toggled(chip, mask // cuts_count), toggled(cuts, mask % cuts_count)
        return c, k, c * cuts_count + k

    def everyone(boards, act):
        def on_board(i, carry):
            where = boards + i
            for c in range(chip_count):
                for k in range(cuts_count):
                    @pl.when((where != board) | (chip != c) | (cuts != k))
                    def _(c=c, k=k):
                        act((c, where, k))

            return carry

        return lambda count: lax.fori_loop(0, count, on_board, 0)

    def x_copy(i):
        part = pl.ds(i * tile, tile)
        return pltpu.make_async_copy(x_hbm.at[0, part], x_buf.at[part], x_sem.at[i])

    rows_copy = pltpu.make_async_copy(rows_hbm.at[0], rows_ref, in_sem.at[0])
    lower_copy = pltpu.make_async_copy(lower_hbm.at[0], lower, in_sem.at[1])
    head_copy = pltpu.make_async_copy(head_hbm.at[0], head, in_sem.at[2])
    target_copy = pltpu.make_async_copy(target_hbm.at[0], target, in_sem.at[3])
    rows_copy.start()
    lower_copy.start()
    x_copy(0).start()
    head_copy.start()
    target_copy.start()
    for i in range(1, tiles):
        x_copy(i).start()

    barrier = pltpu.get_barrier_semaphore()

    everyone(0, lambda device: pl.semaphore_signal(barrier, inc=1, device_id=device, device_id_type=MESH))(board_count)
    kind = lax.broadcasted_iota(jnp.int32, (CLUSTERS, LANES), 0)
    facts[me] = jnp.where(kind == id_ref[0], count_ref[0].astype(jnp.float32), 0.0)

    rows_copy.wait()
    blocks = pool // LANES
    for step in range(steps):
        rows = rows_ref[step : step + 1, :]
        outer = lax.shift_right_logical(rows, 7)
        inner = lax.bitwise_and(rows, LANES - 1)
        one_outer = (lax.broadcasted_iota(jnp.int32, (blocks, count_rows), 0) == outer).astype(jnp.float32).astype(jnp.bfloat16)
        one_inner = (lax.broadcasted_iota(jnp.int32, (LANES, count_rows), 0) == inner).astype(jnp.float32).astype(jnp.bfloat16)
        table = lax.dot_general(one_inner, one_outer, (((1,), (1,)), ((), ())), preferred_element_type=jnp.float32)
        for j in range(blocks):
            drawn[step, j * LANES : (j + 1) * LANES, :] = jnp.broadcast_to(table[:, j : j + 1], (LANES, LANES))

    head_copy.wait()
    def wide(line):
        return line if columns == LANES else jnp.concatenate([line] * (columns // LANES), axis=1)

    def lanes(j):
        return pl.ds(j * columns, columns)

    here, rest = pl.ds(0, columns), pl.ds(columns, columns)
    for j in range(groups):
        high, low = halves(head[:, lanes(j)])
        w_first[:, lanes(j)] = high
        w_pack[j, :, here] = high
        w_pack[j, :, rest] = low
    lower_copy.wait()
    scale = -LR / count_rows

    def error(step, j, part, h_hi, low_term):
        both = dot(h_hi, w_pack[j])
        err = both[:, :columns] + both[:, columns:] + low_term
        err = err - target[part, lanes(j)].astype(jnp.float32)
        err = err * wide(drawn[step, part, :]) * scale
        e_hi, e_lo = halves(err)
        err_pack[part, here] = e_hi
        err_pack[part, rest] = e_lo

    def first_error(part, h_hi, h_lo):
        low = dot(h_lo, w_first[...])
        for j in range(1, groups):
            low_rest[j - 1, part, :] = low[:, j * columns : (j + 1) * columns]
        error(0, 0, part, h_hi, low[:, :columns])

    def gradient(part):
        both = dot(hid_t_hi[part, :], err_pack[...])
        return both[:, :columns] + both[:, columns:] + dot(hid_t_lo[part, :], err_pack[:, here])

    def keep(part, product):
        h_hi, h_lo = halves(jnp.tanh(product))
        hid_hi[part, :] = h_hi
        hid_lo[part, :] = h_lo
        hid_t_hi[:, part] = h_hi.T
        hid_t_lo[:, part] = h_lo.T
        return h_hi, h_lo

    parts = [pl.ds(i * tile, tile) for i in range(tiles)]
    for i in range(min(WAIT, tiles)):
        x_copy(i).wait()
    kept = None
    for i in range(tiles):
        if i == WAIT:
            for k in range(WAIT, tiles):
                x_copy(k).wait()
        if i == 1:
            target_copy.wait()
        product = dot(x_buf[parts[i], :], lower[...])
        if kept is not None:
            first_error(parts[i - 1], *kept)
        kept = keep(parts[i], product)
    if tiles == 1:
        target_copy.wait()
    first_error(parts[-1], *kept)

    pl.semaphore_wait(barrier, number - 1)

    def tell(device):
        pltpu.make_async_remote_copy(
            src_ref=facts.at[me], dst_ref=facts.at[me], send_sem=fact_send, recv_sem=fact_recv,
            device_id=device, device_id_type=MESH,
        ).start()

    everyone(half - 1, tell)(2)

    def rows_of(k, seat_index):
        return pl.ds(pl.multiple_of(lax.rem(k, chunks // groups) * block + seat_index * share, 8), share)

    def group_of(k):
        return lax.div(k, chunks // groups)

    def columns_of(k):
        return pl.ds(pl.multiple_of(group_of(k) * columns, LANES), columns)

    def give_share(k, mask):
        c, z, peer = seat_of(mask)
        pltpu.make_async_remote_copy(
            src_ref=delta.at[group_of(k), rows_of(k, peer)], dst_ref=inbox.at[k, member],
            send_sem=share_send, recv_sem=share_recv.at[k],
            device_id=(c, hub, z), device_id_type=MESH,
        ).start()

    def give_shares(k):
        @pl.when(is_hub)
        def _():
            inbox[k, member] = delta[group_of(k), rows_of(k, seat), :]

        for mask in far_first(range(plane)):
            if mask > 0:
                give_share(k, mask)
            else:
                @pl.when(jnp.logical_not(is_hub))
                def _():
                    give_share(k, 0)

    grad_rows = min(max(GRAD_ROWS, block), hid)
    row_blocks = chunks // groups
    for j in range(groups):
        for step in range(steps):
            for part in parts:
                if step > 0:
                    error(step, j, part, hid_hi[part, :], dot(hid_lo[part, :], w_pack[j, :, here]))
                elif j > 0:
                    error(step, j, part, hid_hi[part, :], low_rest[j - 1, part, :])
            for i in range(hid // grad_rows):
                part = pl.ds(i * grad_rows, grad_rows)
                value = gradient(part)
                if step > 0:
                    value = value + delta[j, part, :]
                delta[j, part, :] = value
                if step + 1 < steps:
                    high, low = halves(head[part, lanes(j)] + value)
                    w_pack[j, part, here] = high
                    w_pack[j, part, rest] = low
                else:
                    def send(k, carry):
                        give_shares(k)
                        return carry

                    start = j * row_blocks + i * grad_rows // block
                    lax.fori_loop(start, start + grad_rows // block, send, 0)

    def arrived(ref, sem):
        pltpu.make_async_copy(ref, ref, sem).wait()

    moved = pl.ds(0, hid // plane * (plane - 1))

    def pair_copy(k):
        return pltpu.make_async_remote_copy(
            src_ref=own.at[k], dst_ref=other.at[k], send_sem=pair_send.at[k], recv_sem=pair_recv.at[k],
            device_id=(chip, board_count - 1 - hub, cuts), device_id_type=MESH,
        )

    @pl.when(is_hub)
    def _():
        arrived(facts.at[pl.ds(0, number - 1)], fact_recv)
        counts = jnp.sum(facts[...], axis=0)
        inverse = 1.0 / (LR * jnp.maximum(counts, 1.0))
        first = side * members
        for t in range(members):
            chosen[t] = jnp.where(facts[first + t] > 0, inverse, 0.0)

        def add_up(k):
            arrived(inbox.at[k, pl.ds(0, members - 1)], share_recv.at[k])
            sums = [jnp.zeros((share, columns), jnp.float32)] * CLUSTERS
            for t in range(members):
                value = inbox[k, t]
                for c in range(CLUSTERS):
                    sums[c] = sums[c] + wide(facts[first + t, c : c + 1, :]) * value
            for c in range(CLUSTERS):
                own[k, c] = sums[c]
            pair_copy(k).start()

        def give_back(k):
            arrived(other.at[k], pair_recv.at[k])
            total = [own[k, c] + other[k, c] for c in range(CLUSTERS)]
            for t in range(members):
                value = wide(chosen[t, 0:1, :]) * total[0]
                for c in range(1, CLUSTERS):
                    value = value + wide(chosen[t, c : c + 1, :]) * total[c]
                outbox[k, t] = value
            out_ref[0, rows_of(k, seat), columns_of(k)] = outbox[k, member]
            for mask in far_first(range(1, members)):
                c, z, peer = seat_of(mask % plane)
                peer_row = toggled(hub_row, mask // plane)
                pltpu.make_async_remote_copy(
                    src_ref=outbox.at[k, peer_row * plane + peer], dst_ref=out_ref.at[0, rows_of(k, seat), columns_of(k)],
                    send_sem=back_send, recv_sem=back_recv,
                    device_id=(c, side * half + peer_row, z), device_id_type=MESH,
                ).start()

        lag = min(LAG, chunks)

        def first_ticks(k, carry):
            add_up(k)
            return carry

        def ticks(k, carry):
            add_up(k)
            give_back(k - lag)
            return carry

        def last_ticks(k, carry):
            give_back(k)
            return carry

        lax.fori_loop(0, lag, first_ticks, 0)
        lax.fori_loop(lag, chunks, ticks, 0)
        lax.fori_loop(chunks - lag, chunks, last_ticks, 0)
        arrived(out_ref.at[0, moved], back_recv)

    @pl.when(jnp.logical_not(is_hub))
    def _():
        arrived(out_ref.at[0], back_recv)

    @pl.when(is_hub)
    def _():
        arrived(delta.at[:, moved], share_send)
        arrived(facts.at[pl.ds(0, 2 * plane - 1)], fact_send)
        for k in range(chunks):
            arrived(own.at[k], pair_send.at[k])
        arrived(outbox.at[:, pl.ds(0, members - 1)], back_send)

    @pl.when(jnp.logical_not(is_hub))
    def _():
        arrived(delta, share_send)
        arrived(facts.at[pl.ds(0, 2 * plane)], fact_send)


def federated_round(sizes, features, targets, lower_weight, head_weight, batch_rows, sample_counts, cluster_ids):
    pool, features_in = features.shape[1:]
    hid, width = head_weight.shape[1:]
    steps, count_rows = batch_rows.shape[1:]
    plane = sizes[0] * sizes[2]
    number = plane * sizes[1]
    members = number // 2
    share = min(SHARE, hid // plane)
    columns = min(COLUMNS, width)
    groups = width // columns
    chunks = hid // (plane * share) * (width // columns)
    tiles = pool // min(TILE, pool)
    vmem = pl.BlockSpec(memory_space=pltpu.VMEM)
    smem = pl.BlockSpec(memory_space=pltpu.SMEM)
    hbm = pl.BlockSpec(memory_space=pltpu.HBM)
    half_type, full_type = jnp.bfloat16, jnp.float32
    one, many = pltpu.SemaphoreType.DMA, pltpu.SemaphoreType.DMA((chunks,))
    return pl.pallas_call(
        functools.partial(round_kernel, sizes),
        name="federated_round",
        out_shape=jax.ShapeDtypeStruct((1, hid, width), full_type),
        in_specs=[hbm] * 5 + [smem] * 2,
        out_specs=vmem,
        scratch_shapes=[
            pltpu.VMEM((pool, features_in), half_type),
            pltpu.VMEM((features_in, hid), half_type),
            pltpu.VMEM((pool, width), half_type),
            pltpu.VMEM((hid, width), full_type),
            pltpu.VMEM((steps, count_rows), jnp.int32),
            pltpu.VMEM((pool, hid), half_type),
            pltpu.VMEM((pool, hid), half_type),
            pltpu.VMEM((hid, pool), half_type),
            pltpu.VMEM((hid, pool), half_type),
            pltpu.VMEM((steps, pool, LANES), full_type),
            pltpu.VMEM((hid, width), half_type),
            pltpu.VMEM((groups, hid, 2 * columns), half_type),
            pltpu.VMEM((max(1, groups - 1), pool, columns), full_type),
            pltpu.VMEM((pool, 2 * columns), half_type),
            pltpu.VMEM((groups, hid, columns), full_type),
            pltpu.VMEM((number, CLUSTERS, LANES), full_type),
            pltpu.VMEM((members, CLUSTERS, LANES), full_type),
            pltpu.VMEM((chunks, members, share, columns), full_type),
            pltpu.VMEM((chunks, CLUSTERS, share, columns), full_type),
            pltpu.VMEM((chunks, CLUSTERS, share, columns), full_type),
            pltpu.VMEM((chunks, members, share, columns), full_type),
            pltpu.SemaphoreType.DMA((tiles,)),
            pltpu.SemaphoreType.DMA((4,)),
            one, one, one, many, many, many, one, one,
        ],
        compiler_params=pltpu.CompilerParams(collective_id=0, has_side_effects=True, vmem_limit_bytes=LIMIT * 2**20),
    )(features, lower_weight, targets, head_weight, batch_rows, sample_counts, cluster_ids)


def solution(mesh):
    sizes = (mesh.shape["chip"], mesh.shape["board"], mesh.shape["cuts"])
    rows, flat = P(("chip", "board", "cuts"), None, None), P(("chip", "board", "cuts"))
    return jax.shard_map(
        functools.partial(federated_round, sizes),
        mesh=mesh,
        in_specs=(rows, rows, rows, rows, rows, flat, flat),
        out_specs=rows,
        check_vma=False,
    )
```
